32 devices in a mesh: slab: 16 (over z, y, x), feat: 2 (over core).
Axes of the slice: x: 2, y: 2, z: 4, core: 2. Of those that a mesh axis runs over, the one named last changes fastest.
Arguments:
- states: float32 [40, 8192], P(None, ('slab', 'feat')), may hold values from -6 to 6
- inputs: float32 [8192], P(('slab', 'feat')), may hold values from -4 to 4
- targets: float32 [40, 8192], P(None, ('slab', 'feat')), may hold values from -4 to 4
Outputs:
- local_operators: float32 [16, 40, 862], P('slab', 'feat')
- scaled_duals: float32 [16, 40, 862], P('slab', 'feat')
- consensus: float32 [40, 862], P('feat')
- residual_history: float32 [2, 2], replicated
The draws below stay inside these ranges and needn't reach their ends.
All inputs are finite; a program needn't handle non-finite values.
Results may differ from the reference program's by a relative error of at most 0.0003.
Values sent between devices are 32-bit elements; how exact they have to be, the bound alone decides.
No kernel may reach another device: no remote copies, remote signals or barrier semaphores. Data moves between devices by JAX's collectives and lax.ppermute only.
A program may use at most 64 MiB of HBM per device.

```python
import jax
import jax.numpy as jnp
from jax import lax

R = 40
ITERS = 2
FEATS = 862
SNAPS = 8192
N_SLAB = 16


def joint_draw(key):
    folded = jax.random.fold_in(key, 9031)
    streams = jax.random.split(folded, 10)
    slab_rows = SNAPS // N_SLAB
    slab_scale = jax.random.uniform(streams[0], (N_SLAB,), minval=0.7, maxval=1.4)
    unit_draw = jnp.clip(jax.random.normal(streams[1], (R, N_SLAB, slab_rows)), -4.0, 4.0)
    states = unit_draw * slab_scale[None, :, None]
    forcing = jnp.clip(jax.random.normal(streams[2], (N_SLAB, slab_rows)), -4.0, 4.0)
    root = R ** 0.5
    linear = jax.random.normal(streams[3], (R, R)) / root
    slab_drift = 0.6 * jax.random.normal(streams[4], (N_SLAB, R, R)) / root
    square_map = 0.3 * jax.random.normal(streams[5], (R, R)) / root
    mixed_map = 0.3 * jax.random.normal(streams[6], (R, R)) / root
    input_gain = jax.random.normal(streams[7], (R,))
    offset = jax.random.normal(streams[8], (R,))
    noise_part = 0.3 * jax.random.normal(streams[9], (R, N_SLAB, slab_rows))
    signal = jnp.einsum('ij,jsk->isk', linear, states)
    signal = signal + jnp.einsum('sij,jsk->isk', slab_drift, states)
    signal = signal + jnp.einsum('ij,jsk->isk', square_map, states * states)
    signal = signal + jnp.einsum('ij,jsk->isk', mixed_map, states * jnp.roll(states, 1, axis=0))
    signal = signal + input_gain[:, None, None] * forcing[None] + offset[:, None, None] + noise_part
    targets = 4.0 * jnp.tanh(signal / 4.0)
    return (states.reshape(R, SNAPS), forcing.reshape(SNAPS), targets.reshape(R, SNAPS))


def draw_states(key, part):
    return joint_draw(key)[0].astype(jnp.float32)


def draw_inputs(key, part):
    return joint_draw(key)[1].astype(jnp.float32)


def draw_targets(key, part):
    return joint_draw(key)[2].astype(jnp.float32)


def setup_inputs(seed: int = 0) -> dict:
    streams_of = jax.random.split(jax.random.key(seed), 4)
    return {
        "states": draw_states(jax.random.fold_in(streams_of[3], 71), 0),
        "inputs": draw_inputs(jax.random.fold_in(streams_of[3], 71), 0),
        "targets": draw_targets(jax.random.fold_in(streams_of[3], 71), 0),
    }


penalty = 1.0

def features(states, inputs):
    reduced = states.shape[0]
    blocks = [states]
    for column in range(reduced):
        blocks.append(states[column:column + 1] * states[column:])
    blocks.append(inputs[None, :])
    blocks.append(jnp.ones_like(inputs)[None, :])
    return jnp.concatenate(blocks, 0)

def reference(states, inputs, targets):
    reduced = states.shape[0]
    slab_rows = states.shape[1] // N_SLAB
    slab_states = states.reshape(reduced, N_SLAB, slab_rows).transpose(1, 0, 2)
    slab_targets = targets.reshape(reduced, N_SLAB, slab_rows).transpose(1, 0, 2)
    slab_inputs = inputs.reshape(N_SLAB, slab_rows)

    def local_solve(packed):
        part_states, part_inputs, part_targets, shifted = packed
        design = features(part_states, part_inputs)
        gram_matrix = jnp.dot(design.astype(jnp.float32), design.T.astype(jnp.float32), precision=lax.Precision.HIGHEST, preferred_element_type=jnp.float32) / slab_rows
        cross = jnp.dot(part_targets.astype(jnp.float32), design.T.astype(jnp.float32), precision=lax.Precision.HIGHEST, preferred_element_type=jnp.float32) / slab_rows
        system = gram_matrix + penalty * jnp.eye(design.shape[0], dtype=jnp.float32)
        return jnp.linalg.solve(system, (cross + penalty * shifted).T).T
    width = FEATS
    consensus = jnp.zeros((reduced, width), jnp.float32)
    duals = jnp.zeros((N_SLAB, reduced, width), jnp.float32)
    primal_list = []
    dual_list = []
    operators = duals
    for sweep in range(ITERS):
        operators = lax.map(local_solve, (slab_states, slab_inputs, slab_targets, consensus[None] - duals))
        updated = lax.optimization_barrier(jnp.sum(operators + duals, 0)) / N_SLAB
        duals = duals + operators - updated[None]
        primal_list.append(jnp.sum(jnp.square(operators - updated[None])))
        dual_list.append(N_SLAB * penalty * penalty * jnp.sum(jnp.square(updated - consensus)))
        consensus = updated
    history = jnp.stack([jnp.stack(primal_list), jnp.stack(dual_list)])
    return (operators, duals, consensus, jnp.sqrt(history / (N_SLAB * reduced * width)))
```

```python
import jax
import jax.numpy as jnp
from jax import lax
from jax.experimental import pallas as pl
from jax.experimental.pallas import tpu as pltpu
from jax.sharding import PartitionSpec as P

penalty = 1.0
F32 = jnp.float32
BF16 = jnp.bfloat16
NN = (((1,), (0,)), ((), ()))
NT = (((1,), (1,)), ((), ()))
TN = (((0,), (0,)), ((), ()))


def mxu(left, right, dims):
    return lax.dot_general(left, right, dims, preferred_element_type=F32)


def split(value):
    high = value.astype(BF16)
    return high, (value - high.astype(F32)).astype(BF16)


def product3(left, right, dims):
    left_high, left_low = left
    right_high, right_low = right
    return mxu(left_high, right_high, dims) + (mxu(left_high, right_low, dims) + mxu(left_low, right_high, dims))


def product(left, right, dims):
    return lax.dot_general(left, right, dims, precision=lax.Precision.HIGHEST, preferred_element_type=F32)


def unit(size):
    return (lax.broadcasted_iota(jnp.int32, (size, size), 0) == lax.broadcasted_iota(jnp.int32, (size, size), 1)).astype(F32)


def refined(right_side, high, low, inverse, rounds):
    inverse_high, inverse_low = inverse
    answer = product3(split(right_side), inverse, NN)
    for _ in range(rounds):
        gap = right_side - product3(split(answer), (high, low), NN)
        answer = answer + mxu(gap.astype(BF16), inverse_high, NN)
    return answer


def first_kernel(states, inputs, targets, operator, phi_high, phi_low, kernel_high, kernel_low, inverse_high, inverse_low, phi, inverse):
    reduced, rows = states.shape
    x = states[...]
    u = inputs[...]
    width = phi.shape[0]
    offset = 0
    phi[0:reduced, :] = x
    offset = reduced
    for column in range(reduced):
        count = reduced - column
        phi[offset : offset + count, :] = x[column : column + 1] * x[column:]
        offset += count
    phi[offset : offset + 1, :] = u
    phi[offset + 1 : offset + 2, :] = jnp.ones_like(u)
    phi[offset + 2 :, :] = jnp.zeros((width - offset - 2, rows), F32)
    whole = phi[...]
    phi_high[...] = whole.astype(BF16)
    phi_low[...] = (whole - whole.astype(BF16).astype(F32)).astype(BF16)
    scale = 1.0 / (rows * penalty)
    inner = product(x, x, TN)
    squares = product(x * x, x * x, TN)
    ends = jnp.concatenate([u, jnp.ones_like(u), jnp.zeros((6, rows), F32)], 0)
    system = inner + 0.5 * (inner * inner + squares) + product(ends, ends, TN)
    identity = unit(rows)
    system = system * scale + identity
    bound = jnp.max(jnp.sum(jnp.abs(system), axis=0))
    high = system.astype(BF16)
    kernel_high[...] = high
    kernel_low[...] = (system - high.astype(F32)).astype(BF16)
    mu = 2.0 / (1.0 + bound)
    delta = (bound - 1.0) / (bound + 1.0)
    inverse[...] = mu * (2.0 * identity - mu * system)
    low_end = 1.0 - delta * delta

    def coarse_more(carry):
        step, low_end = carry
        return jnp.logical_and(low_end < 0.9, step < 40)

    def coarse(carry):
        step, low_end = carry
        s = 2.0 / (1.0 + low_end)
        guess = inverse[...]
        guess_high = guess.astype(BF16)
        gap = unit(rows) - s * mxu(kernel_high[...], guess_high, NN)
        inverse[...] = s * (guess + mxu(guess_high, gap.astype(BF16), NN))
        shrink = (1.0 - low_end) / (1.0 + low_end)
        return step + 1, 1.0 - shrink * shrink

    lax.while_loop(coarse_more, coarse, (jnp.int32(0), low_end))

    def residual():
        return unit(rows) - product3((kernel_high[...], kernel_low[...]), split(inverse[...]), NN)

    start_gap = residual()
    start = jnp.sum(start_gap * start_gap)
    bad = jnp.logical_not(start < 0.5)

    @pl.when(bad)
    def _():
        inverse[...] = mu * unit(rows)

    @pl.when(jnp.logical_not(bad))
    def _():
        guess = inverse[...]
        inverse[...] = guess + product3(split(guess), split(start_gap), NN)

    def fine_more(carry):
        step, size = carry
        return jnp.logical_and(size > 1e-3, step < 60)

    def fine(carry):
        step, _ = carry
        gap = residual()
        guess = inverse[...]
        inverse[...] = guess + product3(split(guess), split(gap), NN)
        return step + 1, jnp.sum(gap * gap)

    lax.while_loop(fine_more, fine, (jnp.int32(0), jnp.where(bad, 1.0, start)))
    found_high, found_low = split(inverse[...])
    inverse_high[...] = found_high
    inverse_low[...] = found_low
    answer = refined(targets[...] * scale, kernel_high[...], kernel_low[...], (found_high, found_low), 1)
    operator[...] = product3(split(answer), (phi_high[...], phi_low[...]), NT)


def second_kernel(slabs, features, half_rows, targets, operator, total, phi_high, phi_low, kernel_high, kernel_low, inverse_high, inverse_low, mean_out, next_operator, summand):
    rows = targets.shape[1]
    scale = 1.0 / (rows * penalty)
    first = operator[...]
    mean = total[...] / slabs
    duals = first - mean
    shifted = mean - duals
    phi = (phi_high[...], phi_low[...])
    kernel = (kernel_high[...], kernel_low[...])
    right_side = (targets[...] - product3(split(shifted), phi, NN)) * scale
    answer = refined(right_side, kernel[0], kernel[1], (inverse_high[...], inverse_low[...]), 1)
    second = shifted + product3(split(answer), phi, NT)
    mean_out[...] = mean
    next_operator[...] = second
    primal = jnp.sum(duals * duals)
    moved = second - mean
    spread = jnp.sum(moved * moved)
    row = lax.broadcasted_iota(jnp.int32, first.shape, 0)
    column = lax.broadcasted_iota(jnp.int32, first.shape, 1)
    extra = jnp.where(column == 0, primal, jnp.where(column == 1, spread, 0.0))
    summand[...] = jnp.where(row == half_rows, extra, second + duals)


def slab_sum(value, slab_count):
    step = 1
    while step < slab_count:
        pairs = [(i, i ^ step) for i in range(slab_count)]
        value = value + lax.ppermute(value, "slab", pairs)
        step *= 2
    return value


def shards(states, inputs, targets):
    reduced, part = states.shape
    feat_count = lax.axis_size("feat")
    slab_count = lax.axis_size("slab")
    half_rows = reduced // feat_count
    rows = part * feat_count
    features = reduced + reduced * (reduced + 1) // 2 + 2
    width = (features + 127) // 128 * 128
    height = (half_rows // 8 + 1) * 8
    core = lax.axis_index("feat")
    swap = [(i, (i + 1) % feat_count) for i in range(feat_count)]
    own = lax.dynamic_slice_in_dim(targets, core * half_rows, half_rows, 0)
    theirs = lax.dynamic_slice_in_dim(targets, (1 - core) * half_rows, half_rows, 0)
    packed = jnp.concatenate([states, theirs, inputs[None]], 0)
    other = lax.ppermute(packed, "feat", swap)
    all_states = jnp.concatenate([states, other[:reduced]], 1)
    all_inputs = jnp.concatenate([inputs[None], other[reduced + half_rows :]], 1)
    picked = jnp.concatenate([own, other[reduced : reduced + half_rows]], 1)
    picked = jnp.pad(picked, ((0, height - half_rows), (0, 0)))
    shape = jax.ShapeDtypeStruct
    flat = shape((height, width), F32)
    operator, *kept = pl.pallas_call(
        first_kernel,
        out_shape=(flat, shape((width, rows), BF16), shape((width, rows), BF16)) + (shape((rows, rows), BF16),) * 4,
        scratch_shapes=[pltpu.VMEM((width, rows), F32), pltpu.VMEM((rows, rows), F32)],
        name="first_solve",
    )(all_states, all_inputs, picked)
    total = slab_sum(operator, slab_count)

    def second(*refs):
        second_kernel(slab_count, features, half_rows, *refs)

    mean, second_operator, summand = pl.pallas_call(second, out_shape=(flat, flat, flat), name="second_solve")(
        picked, operator, total, *kept
    )
    total = slab_sum(summand, slab_count)
    keep = lambda value: value[:half_rows, :features]
    consensus = keep(total) / slab_count
    before = keep(mean)
    duals = keep(operator) - before + keep(second_operator) - consensus
    first_dual = slab_count * penalty * penalty * jnp.sum(jnp.square(before))
    moved = slab_count * jnp.sum(jnp.square(consensus - before))
    sums = jnp.stack([total[half_rows, 0], total[half_rows, 1] - moved, first_dual, penalty * penalty * moved])
    sums = sums + lax.ppermute(sums, "feat", swap)
    history = jnp.maximum(sums, 0.0).reshape(2, 2)
    residual_history = jnp.sqrt(history / (slab_count * reduced * features))
    return (keep(second_operator)[None], duals[None], consensus, residual_history)


def solution(mesh):
    in_specs = (P(None, ("slab", "feat")), P(("slab", "feat")), P(None, ("slab", "feat")))
    out_specs = (P("slab", "feat", None), P("slab", "feat", None), P("feat", None), P())
    return jax.shard_map(shards, mesh=mesh, in_specs=in_specs, out_specs=out_specs, check_vma=False)
```

```python
import jax
import jax.numpy as jnp
from jax import lax
from jax.experimental import pallas as pl
from jax.experimental.pallas import tpu as pltpu
from jax.sharding import PartitionSpec as P

penalty = 1.0
F32 = jnp.float32
BF16 = jnp.bfloat16
NN = (((1,), (0,)), ((), ()))
NT = (((1,), (1,)), ((), ()))
TN = (((0,), (0,)), ((), ()))


def mxu(left, right, dims):
    return lax.dot_general(left, right, dims, preferred_element_type=F32)


def split(value):
    high = value.astype(BF16)
    return high, (value - high.astype(F32)).astype(BF16)


def product3(left, right, dims):
    left_high, left_low = left
    right_high, right_low = right
    return mxu(left_high, right_high, dims) + (mxu(left_high, right_low, dims) + mxu(left_low, right_high, dims))


def product(left, right, dims):
    return lax.dot_general(left, right, dims, precision=lax.Precision.HIGHEST, preferred_element_type=F32)


def unit(size):
    return (lax.broadcasted_iota(jnp.int32, (size, size), 0) == lax.broadcasted_iota(jnp.int32, (size, size), 1)).astype(F32)


def refined(right_side, high, low, inverse, rounds):
    inverse_high, inverse_low = inverse
    answer = product3(split(right_side), inverse, NN)
    for _ in range(rounds):
        gap = right_side - product3(split(answer), (high, low), NN)
        answer = answer + mxu(gap.astype(BF16), inverse_high, NN)
    return answer


def first_kernel(states, inputs, targets, operator, phi_high, phi_low, kernel_high, kernel_low, inverse_high, inverse_low, phi, inverse):
    reduced, rows = states.shape
    x = states[...]
    u = inputs[...]
    width = phi.shape[0]
    offset = 0
    phi[0:reduced, :] = x
    offset = reduced
    for column in range(reduced):
        count = reduced - column
        phi[offset : offset + count, :] = x[column : column + 1] * x[column:]
        offset += count
    phi[offset : offset + 1, :] = u
    phi[offset + 1 : offset + 2, :] = jnp.ones_like(u)
    phi[offset + 2 :, :] = jnp.zeros((width - offset - 2, rows), F32)
    whole = phi[...]
    phi_high[...] = whole.astype(BF16)
    phi_low[...] = (whole - whole.astype(BF16).astype(F32)).astype(BF16)
    scale = 1.0 / (rows * penalty)
    inner = product(x, x, TN)
    squares = product(x * x, x * x, TN)
    ends = jnp.concatenate([u, jnp.ones_like(u), jnp.zeros((6, rows), F32)], 0)
    system = inner + 0.5 * (inner * inner + squares) + product(ends, ends, TN)
    identity = unit(rows)
    system = system * scale + identity
    bound = jnp.max(jnp.sum(jnp.abs(system), axis=0))
    high = system.astype(BF16)
    kernel_high[...] = high
    kernel_low[...] = (system - high.astype(F32)).astype(BF16)
    mu = 2.0 / (1.0 + bound)
    delta = (bound - 1.0) / (bound + 1.0)
    inverse[...] = mu * (2.0 * identity - mu * system)
    low_end = 1.0 - delta * delta

    def coarse_more(carry):
        step, low_end = carry
        return jnp.logical_and(low_end < 0.99, step < 40)

    def coarse(carry):
        step, low_end = carry
        s = 2.0 / (1.0 + low_end)
        guess = inverse[...]
        guess_high = guess.astype(BF16)
        gap = unit(rows) - s * mxu(kernel_high[...], guess_high, NN)
        inverse[...] = s * (guess + mxu(guess_high, gap.astype(BF16), NN))
        shrink = (1.0 - low_end) / (1.0 + low_end)
        return step + 1, 1.0 - shrink * shrink

    lax.while_loop(coarse_more, coarse, (jnp.int32(0), low_end))

    def residual():
        return unit(rows) - product3((kernel_high[...], kernel_low[...]), split(inverse[...]), NN)

    start_gap = residual()
    start = jnp.sum(start_gap * start_gap)
    bad = jnp.logical_not(start < 0.9)

    @pl.when(bad)
    def _():
        inverse[...] = mu * unit(rows)

    @pl.when(jnp.logical_not(bad))
    def _():
        guess = inverse[...]
        inverse[...] = guess + product3(split(guess), split(start_gap), NN)

    def fine_more(carry):
        step, size = carry
        return jnp.logical_and(size > 5e-3, step < 60)

    def fine(carry):
        step, _ = carry
        gap = residual()
        guess = inverse[...]
        inverse[...] = guess + product3(split(guess), split(gap), NN)
        return step + 1, jnp.sum(gap * gap)

    lax.while_loop(fine_more, fine, (jnp.int32(0), jnp.where(bad, 1.0, start)))
    found_high, found_low = split(inverse[...])
    inverse_high[...] = found_high
    inverse_low[...] = found_low
    answer = refined(targets[...] * scale, kernel_high[...], kernel_low[...], (found_high, found_low), 1)
    operator[...] = product3(split(answer), (phi_high[...], phi_low[...]), NT)


def second_kernel(slabs, features, half_rows, targets, operator, total, phi_high, phi_low, kernel_high, kernel_low, inverse_high, inverse_low, mean_out, next_operator, summand):
    rows = targets.shape[1]
    scale = 1.0 / (rows * penalty)
    first = operator[...]
    mean = total[...] / slabs
    duals = first - mean
    shifted = mean - duals
    phi = (phi_high[...], phi_low[...])
    kernel = (kernel_high[...], kernel_low[...])
    right_side = (targets[...] - product3(split(shifted), phi, NN)) * scale
    answer = refined(right_side, kernel[0], kernel[1], (inverse_high[...], inverse_low[...]), 1)
    second = shifted + product3(split(answer), phi, NT)
    mean_out[...] = mean
    next_operator[...] = second
    primal = jnp.sum(duals * duals)
    moved = second - mean
    spread = jnp.sum(moved * moved)
    row = lax.broadcasted_iota(jnp.int32, first.shape, 0)
    column = lax.broadcasted_iota(jnp.int32, first.shape, 1)
    extra = jnp.where(column == 0, primal, jnp.where(column == 1, spread, 0.0))
    summand[...] = jnp.where(row == half_rows, extra, second + duals)


def slab_sum(value, slab_count):
    def from_peer(distance):
        return lax.ppermute(value, "slab", [(i, i ^ distance) for i in range(slab_count)])

    step = 1
    while step < slab_count:
        if slab_count % (4 * step) == 0:
            near, far, both = (from_peer(step * turn) for turn in (1, 2, 3))
            value = (value + near) + (far + both)
            step *= 4
        else:
            value = value + from_peer(step)
            step *= 2
    return value


def shards(states, inputs, targets):
    reduced, part = states.shape
    feat_count = lax.axis_size("feat")
    slab_count = lax.axis_size("slab")
    half_rows = reduced // feat_count
    rows = part * feat_count
    features = reduced + reduced * (reduced + 1) // 2 + 2
    width = (features + 127) // 128 * 128
    height = (half_rows // 8 + 1) * 8
    core = lax.axis_index("feat")
    swap = [(i, (i + 1) % feat_count) for i in range(feat_count)]
    own = lax.dynamic_slice_in_dim(targets, core * half_rows, half_rows, 0)
    theirs = lax.dynamic_slice_in_dim(targets, (1 - core) * half_rows, half_rows, 0)
    packed = jnp.concatenate([states, theirs, inputs[None]], 0)
    other = lax.ppermute(packed, "feat", swap)
    all_states = jnp.concatenate([states, other[:reduced]], 1)
    all_inputs = jnp.concatenate([inputs[None], other[reduced + half_rows :]], 1)
    picked = jnp.concatenate([own, other[reduced : reduced + half_rows]], 1)
    picked = jnp.pad(picked, ((0, height - half_rows), (0, 0)))
    shape = jax.ShapeDtypeStruct
    flat = shape((height, width), F32)
    operator, *kept = pl.pallas_call(
        first_kernel,
        out_shape=(flat, shape((width, rows), BF16), shape((width, rows), BF16)) + (shape((rows, rows), BF16),) * 4,
        scratch_shapes=[pltpu.VMEM((width, rows), F32), pltpu.VMEM((rows, rows), F32)],
        name="first_solve",
    )(all_states, all_inputs, picked)
    total = slab_sum(operator, slab_count)

    def second(*refs):
        second_kernel(slab_count, features, half_rows, *refs)

    mean, second_operator, summand = pl.pallas_call(second, out_shape=(flat, flat, flat), name="second_solve")(
        picked, operator, total, *kept
    )
    total = slab_sum(summand, slab_count)
    keep = lambda value: value[:half_rows, :features]
    consensus = keep(total) / slab_count
    before = keep(mean)
    duals = keep(operator) - before + keep(second_operator) - consensus
    first_dual = slab_count * penalty * penalty * jnp.sum(jnp.square(before))
    moved = slab_count * jnp.sum(jnp.square(consensus - before))
    sums = jnp.stack([total[half_rows, 0], total[half_rows, 1] - moved, first_dual, penalty * penalty * moved])
    sums = sums + lax.ppermute(sums, "feat", swap)
    history = jnp.maximum(sums, 0.0).reshape(2, 2)
    residual_history = jnp.sqrt(history / (slab_count * reduced * features))
    return (keep(second_operator)[None], duals[None], consensus, residual_history)


def solution(mesh):
    in_specs = (P(None, ("slab", "feat")), P(("slab", "feat")), P(None, ("slab", "feat")))
    out_specs = (P("slab", "feat", None), P("slab", "feat", None), P("feat", None), P())
    return jax.shard_map(shards, mesh=mesh, in_specs=in_specs, out_specs=out_specs, check_vma=False)
```

```python
import jax
import jax.numpy as jnp
from jax import lax
from jax.experimental import pallas as pl
from jax.experimental.pallas import tpu as pltpu
from jax.sharding import PartitionSpec as P

penalty = 1.0
F32 = jnp.float32
BF16 = jnp.bfloat16
NN = (((1,), (0,)), ((), ()))
NT = (((1,), (1,)), ((), ()))
TN = (((0,), (0,)), ((), ()))


def mxu(left, right, dims):
    return lax.dot_general(left, right, dims, preferred_element_type=F32)


def split(value):
    high = value.astype(BF16)
    return high, (value - high.astype(F32)).astype(BF16)


def product3(left, right, dims):
    left_high, left_low = left
    right_high, right_low = right
    return mxu(left_high, right_high, dims) + (mxu(left_high, right_low, dims) + mxu(left_low, right_high, dims))


def product(left, right, dims):
    return lax.dot_general(left, right, dims, precision=lax.Precision.HIGHEST, preferred_element_type=F32)


def unit(size):
    return (lax.broadcasted_iota(jnp.int32, (size, size), 0) == lax.broadcasted_iota(jnp.int32, (size, size), 1)).astype(F32)


def refined(right_side, high, low, inverse, rounds):
    inverse_high, inverse_low = inverse
    answer = product3(split(right_side), inverse, NN)
    for _ in range(rounds):
        gap = right_side - product3(split(answer), (high, low), NN)
        answer = answer + mxu(gap.astype(BF16), inverse_high, NN)
    return answer


def first_kernel(half_rows, core, mine, other, targets, operator, phi_high, phi_low, kernel_high, kernel_low, inverse_high, inverse_low, phi, inverse):
    reduced = 2 * half_rows
    rows = 2 * mine.shape[1]
    both = lambda start, stop: jnp.concatenate([mine[start:stop, :], other[start:stop, :]], 1)
    x = both(0, reduced)
    u = both(2 * reduced, 2 * reduced + 1)
    aims = both(reduced, 2 * reduced)
    picked = jnp.where(core[0] == 0, aims[:half_rows], aims[half_rows:])
    targets[...] = jnp.zeros(targets.shape, F32)
    targets[0:half_rows, :] = picked
    width = phi.shape[0]
    offset = 0
    phi[0:reduced, :] = x
    offset = reduced
    for column in range(reduced):
        count = reduced - column
        phi[offset : offset + count, :] = x[column : column + 1] * x[column:]
        offset += count
    phi[offset : offset + 1, :] = u
    phi[offset + 1 : offset + 2, :] = jnp.ones_like(u)
    phi[offset + 2 :, :] = jnp.zeros((width - offset - 2, rows), F32)
    whole = phi[...]
    phi_high[...] = whole.astype(BF16)
    phi_low[...] = (whole - whole.astype(BF16).astype(F32)).astype(BF16)
    scale = 1.0 / (rows * penalty)
    inner = product(x, x, TN)
    squares = product(x * x, x * x, TN)
    ends = jnp.concatenate([u, jnp.ones_like(u), jnp.zeros((6, rows), F32)], 0)
    system = inner + 0.5 * (inner * inner + squares) + product(ends, ends, TN)
    identity = unit(rows)
    system = system * scale + identity
    bound = jnp.max(jnp.sum(jnp.abs(system), axis=0))
    high = system.astype(BF16)
    kernel_high[...] = high
    kernel_low[...] = (system - high.astype(F32)).astype(BF16)
    mu = 2.0 / (1.0 + bound)
    delta = (bound - 1.0) / (bound + 1.0)
    inverse[...] = mu * (2.0 * identity - mu * system)
    low_end = 1.0 - delta * delta

    def coarse_more(carry):
        step, low_end = carry
        return jnp.logical_and(low_end < 0.99, step < 40)

    def coarse(carry):
        step, low_end = carry
        s = 2.0 / (1.0 + low_end)
        guess = inverse[...]
        guess_high = guess.astype(BF16)
        gap = unit(rows) - s * mxu(kernel_high[...], guess_high, NN)
        inverse[...] = s * (guess + mxu(guess_high, gap.astype(BF16), NN))
        shrink = (1.0 - low_end) / (1.0 + low_end)
        return step + 1, 1.0 - shrink * shrink

    lax.while_loop(coarse_more, coarse, (jnp.int32(0), low_end))

    def residual():
        return unit(rows) - product3((kernel_high[...], kernel_low[...]), split(inverse[...]), NN)

    start_gap = residual()
    start = jnp.sum(start_gap * start_gap)
    bad = jnp.logical_not(start < 0.9)

    @pl.when(bad)
    def _():
        inverse[...] = mu * unit(rows)

    @pl.when(jnp.logical_not(bad))
    def _():
        guess = inverse[...]
        inverse[...] = guess + product3(split(guess), split(start_gap), NN)

    def fine_more(carry):
        step, size = carry
        return jnp.logical_and(size > 5e-3, step < 60)

    def fine(carry):
        step, _ = carry
        gap = residual()
        guess = inverse[...]
        inverse[...] = guess + product3(split(guess), split(gap), NN)
        return step + 1, jnp.sum(gap * gap)

    lax.while_loop(fine_more, fine, (jnp.int32(0), jnp.where(bad, 1.0, start)))
    found_high, found_low = split(inverse[...])
    inverse_high[...] = found_high
    inverse_low[...] = found_low
    answer = refined(targets[...] * scale, kernel_high[...], kernel_low[...], (found_high, found_low), 1)
    operator[...] = product3(split(answer), (phi_high[...], phi_low[...]), NT)


def second_kernel(slabs, features, half_rows, targets, operator, total, phi_high, phi_low, kernel_high, kernel_low, inverse_high, inverse_low, mean_out, next_operator, summand):
    rows = targets.shape[1]
    scale = 1.0 / (rows * penalty)
    first = operator[...]
    mean = total[...] / slabs
    duals = first - mean
    shifted = mean - duals
    phi = (phi_high[...], phi_low[...])
    kernel = (kernel_high[...], kernel_low[...])
    right_side = (targets[...] - product3(split(shifted), phi, NN)) * scale
    answer = refined(right_side, kernel[0], kernel[1], (inverse_high[...], inverse_low[...]), 1)
    second = shifted + product3(split(answer), phi, NT)
    mean_out[...] = mean
    next_operator[...] = second[: next_operator.shape[0], : next_operator.shape[1]]
    primal = jnp.sum(duals * duals)
    moved = second - mean
    spread = jnp.sum(moved * moved)
    row = lax.broadcasted_iota(jnp.int32, first.shape, 0)
    column = lax.broadcasted_iota(jnp.int32, first.shape, 1)
    extra = jnp.where(column == 0, primal, jnp.where(column == 1, spread, 0.0))
    summand[...] = jnp.where(row == half_rows, extra, second + duals)


def closing_kernel(slabs, half_rows, operator, mean, second, total, consensus, duals, sums):
    height, width = consensus.shape
    before = mean[0:height, 0:width]
    latest = total[0:height, 0:width] / slabs
    consensus[...] = latest
    duals[...] = operator[0:height, 0:width] - before + second[...] - latest
    first_dual = slabs * penalty * penalty * jnp.sum(jnp.square(before))
    moved = slabs * jnp.sum(jnp.square(latest - before))
    scalars = total[half_rows : half_rows + 1, 0:128]
    lane = lax.broadcasted_iota(jnp.int32, scalars.shape, 1)
    first_primal = jnp.sum(jnp.where(lane == 0, scalars, 0.0))
    second_primal = jnp.sum(jnp.where(lane == 1, scalars, 0.0)) - moved
    row = lax.broadcasted_iota(jnp.int32, sums.shape, 0)
    column = lax.broadcasted_iota(jnp.int32, sums.shape, 1)
    primal = jnp.where(column == 0, first_primal, second_primal)
    dual = jnp.where(column == 0, first_dual, penalty * penalty * moved)
    sums[...] = jnp.where(row == 0, primal, dual)


def slab_sum(value, slab_count):
    def from_peer(distance):
        return lax.ppermute(value, "slab", [(i, i ^ distance) for i in range(slab_count)])

    step = 1
    while step < slab_count:
        if slab_count % (4 * step) == 0:
            near, far, both = (from_peer(step * turn) for turn in (1, 2, 3))
            value = (value + near) + (far + both)
            step *= 4
        else:
            value = value + from_peer(step)
            step *= 2
    return value


def shards(states, inputs, targets):
    reduced, part = states.shape
    feat_count = lax.axis_size("feat")
    slab_count = lax.axis_size("slab")
    half_rows = reduced // feat_count
    rows = part * feat_count
    features = reduced + reduced * (reduced + 1) // 2 + 2
    width = (features + 127) // 128 * 128
    height = (half_rows // 8 + 1) * 8
    core = lax.axis_index("feat")
    swap = [(i, (i + 1) % feat_count) for i in range(feat_count)]
    packed = jnp.concatenate([states, targets, inputs[None]], 0)
    other = lax.ppermute(packed, "feat", swap)
    shape = jax.ShapeDtypeStruct
    flat = shape((height, width), F32)
    block = shape((half_rows, features), F32)
    whole = pl.BlockSpec(memory_space=pltpu.VMEM)

    def first(*refs):
        first_kernel(half_rows, *refs)

    picked, operator, *kept = pl.pallas_call(
        first,
        out_shape=(shape((height, rows), F32), flat, shape((width, rows), BF16), shape((width, rows), BF16))
        + (shape((rows, rows), BF16),) * 4,
        in_specs=[pl.BlockSpec(memory_space=pltpu.SMEM), whole, whole],
        scratch_shapes=[pltpu.VMEM((width, rows), F32), pltpu.VMEM((rows, rows), F32)],
        name="first_solve",
    )(core.reshape(1).astype(jnp.int32), packed, other)
    total = slab_sum(operator, slab_count)

    def second(*refs):
        second_kernel(slab_count, features, half_rows, *refs)

    mean, second_operator, summand = pl.pallas_call(second, out_shape=(flat, block, flat), name="second_solve")(
        picked, operator, total, *kept
    )
    total = slab_sum(summand, slab_count)

    def closing(*refs):
        closing_kernel(slab_count, half_rows, *refs)

    consensus, duals, sums = pl.pallas_call(closing, out_shape=(block, block, shape((2, 2), F32)), name="closing")(
        operator, mean, second_operator, total
    )
    sums = sums + lax.ppermute(sums, "feat", swap)
    history = jnp.maximum(sums, 0.0)
    residual_history = jnp.sqrt(history / (slab_count * reduced * features))
    return (second_operator[None], duals[None], consensus, residual_history)


def solution(mesh):
    in_specs = (P(None, ("slab", "feat")), P(("slab", "feat")), P(None, ("slab", "feat")))
    out_specs = (P("slab", "feat", None), P("slab", "feat", None), P("feat", None), P())
    return jax.shard_map(shards, mesh=mesh, in_specs=in_specs, out_specs=out_specs, check_vma=False)
```
